32 devices in a mesh: row: 4 (over z), col: 8 (over y, x, core).
Axes of the slice: x: 2, y: 2, z: 4, core: 2. Of those that a mesh axis runs over, the one named last changes fastest.
Arguments:
- response_coeffs: float32 [3, 8192, 1024], P(None, ('row', 'col')), may hold values from -6 to 6
- occupied_coeffs: float32 [8192, 1024], P(('row', 'col')), may hold values from -0.1875 to 0.1875
Outputs:
- density: float32 [3, 8192, 8192], P(None, 'row', 'col')
The draws below stay inside these ranges and needn't reach their ends.
All inputs are finite; a program needn't handle non-finite values.
Results may differ from the reference program's by a relative error of at most 0.0003.
Values sent between devices are 32-bit elements; how exact they have to be, the bound alone decides.
A program may use at most 256 MiB of HBM per device.

```python
import jax
import jax.numpy as jnp
from jax import lax

BASIS = 8192
OCC = 1024
PERTURB = 3


def level_of(key, dims, split, low, top_value):
    gain, own = 1.0, jax.random.fold_in(key, 6)
    for dim, blocks in split:
        heights = jnp.exp(jax.random.uniform(jax.random.fold_in(own, dim), (blocks,), jnp.float32, low / len(split), top_value / len(split)))
        gain = gain * jnp.repeat(heights, dims[dim] // blocks).reshape([-1 if axis == dim else 1 for axis in range(len(dims))])
    return gain


def normal_values(rng, shape, deviation, most, pieces=(), dtype=jnp.bfloat16):
    values = deviation * jax.random.normal(rng, shape, jnp.float32)
    if pieces:
        values = values * level_of(rng, shape, pieces, -0.22, 0.18)
    return jnp.clip(values, -most, most).astype(dtype)


def setup_inputs(seed: int = 0) -> dict:
    keys = jax.random.split(jax.random.key(seed), 3)
    response_coeffs = normal_values(keys[0], (PERTURB, BASIS, OCC), 1.0, 6.0, ((1, 32),), jnp.float32)
    occupied_coeffs = normal_values(keys[1], (BASIS, OCC), OCC ** -0.5, 0.1875, ((0, 32),), jnp.float32)
    return dict(response_coeffs=response_coeffs, occupied_coeffs=occupied_coeffs)


SLICE_PAIRS = ((0, 0), (0, 1), (1, 0))


def split_slices(values):
    leading = lax.optimization_barrier(values.astype(jnp.bfloat16))
    remainder = values - leading.astype(jnp.float32)
    trailing = lax.optimization_barrier(remainder.astype(jnp.bfloat16))
    return [leading, trailing]


def reference(response_coeffs, occupied_coeffs):
    response_slices = split_slices(response_coeffs)
    occupied_slices = split_slices(occupied_coeffs)
    accumulated = jnp.zeros((PERTURB, BASIS, BASIS), jnp.float32)
    for left_index, right_index in SLICE_PAIRS:
        accumulated = accumulated + jnp.einsum(
            "kno,mo->knm",
            response_slices[left_index].astype(jnp.float32),
            occupied_slices[right_index].astype(jnp.float32),
            precision=lax.Precision.HIGHEST,
        )
    return accumulated + jnp.swapaxes(accumulated, 1, 2)
```

```python
import functools

import jax
import jax.numpy as jnp
from jax import lax
from jax.experimental import pallas as pl
from jax.experimental.pallas import tpu as pltpu
from jax.sharding import PartitionSpec as P

SLICE_PAIRS = ((0, 0), (0, 1), (1, 0))


def partner(value, axis, stride):
    mask = 2**stride
    pairs = [(source, source ^ mask) for source in range(lax.axis_size(axis))]
    return lax.ppermute(value, axis, pairs)


def split_slices(values):
    leading = lax.optimization_barrier(values.astype(jnp.bfloat16))
    remainder = values - leading.astype(jnp.float32)
    trailing = lax.optimization_barrier(remainder.astype(jnp.bfloat16))
    return [leading, trailing]


def contribute(row_slices, column_slices, perturbations):
    accumulated = jnp.zeros(
        (perturbations, row_slices[0].shape[1], column_slices[0].shape[1]), jnp.float32
    )
    for left_index, right_index in SLICE_PAIRS:
        forward_term = jnp.einsum(
            "kro,co->krc",
            row_slices[left_index][:perturbations],
            column_slices[right_index][perturbations],
            preferred_element_type=jnp.float32,
        )
        mirror_term = jnp.einsum(
            "ro,kco->krc",
            row_slices[right_index][perturbations],
            column_slices[left_index][:perturbations],
            preferred_element_type=jnp.float32,
        )
        accumulated = accumulated + forward_term + mirror_term
    return accumulated


def relay_columns(stacked, perturbations):
    rows_total = lax.axis_size("row")
    columns_total = lax.axis_size("col")
    col_index = lax.axis_index("col")
    shard_rows = stacked.shape[1]
    orbitals = stacked.shape[2]
    half_rows = shard_rows // 2
    swap_bit = rows_total.bit_length() - 1
    own_first = stacked[:, :half_rows]
    partner_second = partner(stacked[:, half_rows:], "col", swap_bit)
    even_first = col_index // rows_total == 0
    leading = jnp.where(even_first, own_first, partner_second)
    trailing = jnp.where(even_first, partner_second, own_first)
    paired = jnp.concatenate([leading, trailing], axis=1)
    gathered = lax.all_gather(paired, "row", axis=1, tiled=True)
    regrouped = lax.all_to_all(gathered, "col", split_axis=1, concat_axis=1, tiled=True)
    shaped = regrouped.reshape(perturbations + 1, 2, rows_total, half_rows, orbitals)
    flipped = shaped[:, ::-1]
    ordered = jnp.where(col_index % 2 == 0, shaped, flipped)
    return jnp.swapaxes(ordered, 1, 2).reshape(
        perturbations + 1, columns_total * half_rows, orbitals
    )


def shards(response_coeffs, occupied_coeffs):
    perturbations = response_coeffs.shape[0]
    stacked = jnp.concatenate([response_coeffs, occupied_coeffs[None]], axis=0)
    column_panel = relay_columns(stacked, perturbations)
    column_slices = split_slices(column_panel)
    return contribute(
        split_slices(lax.all_gather(stacked, "col", axis=1, tiled=True)),
        column_slices,
        perturbations,
    )


HALVES = 2


def flip(value):
    return value + 1 - 2 * (value % 2)


def across(value):
    return value + 2 - 4 * (value // 2)


def panel_kernel(
    resp, occ, out, rowbuf, colbuf,
    row_lead, row_trail, col_lead, col_trail, stage, tile,
    rx_row, rx_col, tx, stage_sem, tile_sem,
):
    perturbations, shard_rows, orbitals = resp.shape
    kinds = perturbations + 1
    piece = shard_rows // HALVES
    pieces = kinds * HALVES
    early = pieces // 2
    positions = 4 * pieces
    block_rows = tile.shape[2]
    row_blocks = 8 * shard_rows // block_rows
    panel_rows = 8 * shard_rows

    z = lax.axis_index("row")
    planes = lax.axis_size("row")
    column = lax.axis_index("col")
    w, core = column // 2, column % 2
    xq, yq, dq = flip(w), across(w), flip(across(w))
    other = 1 - core
    x_dev, y_dev, p_dev = (z, 2 * xq + core), (z, 2 * yq + core), (z, 2 * w + other)
    up_dev, down_dev = (z + 1, column), (z - 1, column)
    has_up, has_down = z < planes - 1, z > 0
    diagonal = z == w
    match = w // 2 == core
    distance = jnp.where(z > w, z - w, w - z)

    barrier = pltpu.get_barrier_semaphore()

    def greet(device):
        pl.semaphore_signal(barrier, inc=1, device_id=device, device_id_type=pl.DeviceIdType.MESH)

    above, below = (z + 1) % planes, (z + planes - 1) % planes
    for device in (x_dev, y_dev, p_dev, (above, column), (below, column)):
        greet(device)
    pl.semaphore_wait(barrier, 5)

    def row_piece(quarter, lane, j):
        return rowbuf.at[2 * quarter + lane, j // HALVES, pl.ds(pl.multiple_of((j % HALVES) * piece, piece), piece)]

    def col_piece(p):
        i, j = p // pieces, p % pieces
        return colbuf.at[i, j // HALVES, pl.ds(pl.multiple_of((j % HALVES) * piece, piece), piece)]

    def send(source, target, send_sem, recv_sem, device):
        pltpu.make_async_remote_copy(
            src_ref=source, dst_ref=target, send_sem=send_sem, recv_sem=recv_sem,
            device_id=device, device_id_type=pl.DeviceIdType.MESH,
        ).start()

    def send_row(quarter, lane, j, slot, device):
        ref = row_piece(quarter, lane, j)
        send(ref, ref, tx.at[slot], rx_row.at[2 * quarter + lane, j], device)

    def wait_row(quarter, lane, j):
        ref = row_piece(quarter, lane, j)
        pltpu.make_async_copy(ref, ref, rx_row.at[2 * quarter + lane, j]).wait()

    load_resp = pltpu.make_async_copy(resp, stage.at[pl.ds(0, perturbations)], stage_sem.at[0])
    load_occ = pltpu.make_async_copy(occ, stage.at[perturbations], stage_sem.at[1])
    load_resp.start()
    load_occ.start()
    for j in range(pieces):
        k, rows = j // HALVES, pl.ds((j % HALVES) * piece, piece)
        source = resp.at[k, rows] if k < perturbations else occ.at[rows]
        for slot, device in ((0, x_dev), (1, y_dev), (4, p_dev)):
            send(source, row_piece(w, core, j), tx.at[slot], rx_row.at[2 * w + core, j], device)
    load_resp.wait()
    load_occ.wait()
    keep = pltpu.make_async_copy(stage, rowbuf.at[2 * w + core], stage_sem.at[0])
    keep.start()
    keep.wait()

    first = jnp.where(match, w, yq)
    second = flip(first)

    def order(i):
        quarter = jnp.where(i < 2, first, second)
        lane = jnp.where(i % 2 == 0, core, other)
        return quarter, lane

    def emit(source, p):
        @pl.when(has_up & (z >= w))
        def _():
            send(source, col_piece(p), tx.at[5], rx_col.at[p], up_dev)

        @pl.when(has_down & (z <= w))
        def _():
            send(source, col_piece(p), tx.at[6], rx_col.at[p], down_dev)

    def emit_own(p):
        quarter, lane = order(p // pieces)
        emit(row_piece(quarter, lane, p % pieces), p)

    def split_into(value, lead, trail, start):
        leading = value.astype(jnp.bfloat16)
        lead[pl.ds(start, shard_rows), :] = leading
        trail[pl.ds(start, shard_rows), :] = (value - leading.astype(jnp.float32)).astype(jnp.bfloat16)

    def load_stage(source):
        copy = pltpu.make_async_copy(source, stage, stage_sem.at[0])
        copy.start()
        copy.wait()

    def tile_copy(slot, block, start):
        return pltpu.make_async_copy(
            tile.at[slot],
            out.at[:, pl.ds(pl.multiple_of(block * block_rows, block_rows), block_rows),
                   pl.ds(pl.multiple_of(start, shard_rows), shard_rows)],
            tile_sem.at[slot],
        )

    gathered = pieces + early
    convert_at = gathered + 1
    matmul_at = convert_at + 8
    rounds = positions + planes - 1
    hidden = 3 * row_blocks
    tasks = 4 * row_blocks

    def step(t, carry):
        @pl.when(t < pieces)
        def _():
            wait_row(xq, core, t)
            send_row(xq, core, t, 4, p_dev)
            wait_row(yq, core, t)
            send_row(yq, core, t, 4, p_dev)
            wait_row(w, other, t)

            @pl.when(t < early)
            def _():
                send_row(yq, core, t, 2, x_dev)

            @pl.when(t >= early)
            def _():
                send_row(xq, core, t, 3, y_dev)

        @pl.when((t >= 1) & (t < pieces + 1))
        def _():
            wait_row(xq, other, t - 1)
            wait_row(yq, other, t - 1)

        @pl.when((t >= pieces) & (t < gathered))
        def _():
            for shift in (0, early):
                wait_row(dq, core, t - pieces + shift)
                send_row(dq, core, t - pieces + shift, 4, p_dev)

        @pl.when((t >= pieces + 1) & (t < gathered + 1))
        def _():
            for shift in (0, early):
                wait_row(dq, other, t - pieces - 1 + shift)

        @pl.when(diagonal & match & (t < positions // 2))
        def _():
            emit_own(2 * t)
            emit_own(2 * t + 1)

        @pl.when(diagonal & (w // 2 != core) & (t < positions))
        def _():
            emit_own(t)

        @pl.when((z != w) & (t >= distance) & (t < positions + distance))
        def _():
            p = t - distance
            ref = col_piece(p)
            pltpu.make_async_copy(ref, ref, rx_col.at[p]).wait()
            emit(ref, p)

        @pl.when((t >= convert_at) & (t < matmul_at))
        def _():
            shard = t - convert_at
            load_stage(rowbuf.at[shard])

            def convert(k, carry):
                start = pl.multiple_of(k * panel_rows + shard * shard_rows, shard_rows)
                split_into(stage[k], row_lead, row_trail, start)
                return carry

            lax.fori_loop(0, kinds, convert, 0)

        @pl.when(((t >= matmul_at) & (t < matmul_at + hidden)) | (t >= rounds))
        def _():
            task = jnp.where(t >= rounds, t - rounds + hidden, t - matmul_at)
            part, block = task // row_blocks, task % row_blocks
            quarter, lane = order(part)

            @pl.when(block == 0)
            def _():
                @pl.when(diagonal)
                def _():
                    load_stage(rowbuf.at[2 * quarter + lane])

                @pl.when(z != w)
                def _():
                    load_stage(colbuf.at[part])

                def convert(k, carry):
                    split_into(stage[k], col_lead, col_trail, pl.multiple_of(k * shard_rows, shard_rows))
                    return carry

                lax.fori_loop(0, kinds, convert, 0)

            slot = task % 2
            place = (2 * (quarter % 2) + lane) * shard_rows

            @pl.when(task >= 2)
            def _():
                tile_copy(slot, block, place).wait()

            def rows_of(ref, k):
                return ref[pl.ds(pl.multiple_of(k * panel_rows + block * block_rows, block_rows), block_rows), :]

            def columns_of(ref, k):
                return ref[pl.ds(pl.multiple_of(k * shard_rows, shard_rows), shard_rows), :]

            def product(left, right):
                return lax.dot_general(left, right, (((1,), (1,)), ((), ())), preferred_element_type=jnp.float32)

            def perturbation(k, carry):
                total = product(rows_of(row_lead, k), columns_of(col_lead, perturbations))
                total += product(rows_of(row_lead, k), columns_of(col_trail, perturbations))
                total += product(rows_of(row_trail, k), columns_of(col_lead, perturbations))
                total += product(rows_of(row_lead, perturbations), columns_of(col_lead, k))
                total += product(rows_of(row_trail, perturbations), columns_of(col_lead, k))
                total += product(rows_of(row_lead, perturbations), columns_of(col_trail, k))
                tile[slot, k] = total
                return carry

            lax.fori_loop(0, perturbations, perturbation, 0)
            tile_copy(slot, block, place).start()

        return carry

    lax.fori_loop(0, rounds + row_blocks, step, 0)

    for slot in range(2):
        tile_copy(slot, 0, 0).wait()

    def drain(slot, ref):
        pltpu.make_async_copy(ref, ref, tx.at[slot]).wait()

    drain(0, rowbuf.at[0])
    drain(1, rowbuf.at[0])
    drain(2, rowbuf.at[0, pl.ds(0, kinds // 2)])
    drain(3, rowbuf.at[0, pl.ds(0, kinds // 2)])
    drain(4, rowbuf.at[pl.ds(0, 4)])

    @pl.when(has_up & (z >= w))
    def _():
        drain(5, rowbuf.at[pl.ds(0, 4)])

    @pl.when(has_down & (z <= w))
    def _():
        drain(6, rowbuf.at[pl.ds(0, 4)])


def panels(response_coeffs, occupied_coeffs):
    perturbations, shard_rows, orbitals = response_coeffs.shape
    kinds = perturbations + 1
    pieces = kinds * HALVES
    block_rows = 2 * shard_rows
    any_space = pl.BlockSpec(memory_space=pl.ANY)
    float32, bfloat16 = jnp.float32, jnp.bfloat16
    return pl.pallas_call(
        panel_kernel,
        out_shape=(
            jax.ShapeDtypeStruct((perturbations, 8 * shard_rows, 4 * shard_rows), float32),
            jax.ShapeDtypeStruct((8, kinds, shard_rows, orbitals), float32),
            jax.ShapeDtypeStruct((4, kinds, shard_rows, orbitals), float32),
        ),
        in_specs=[any_space] * 2,
        out_specs=(any_space,) * 3,
        scratch_shapes=[
            pltpu.VMEM((kinds * 8 * shard_rows, orbitals), bfloat16),
            pltpu.VMEM((kinds * 8 * shard_rows, orbitals), bfloat16),
            pltpu.VMEM((kinds * shard_rows, orbitals), bfloat16),
            pltpu.VMEM((kinds * shard_rows, orbitals), bfloat16),
            pltpu.VMEM((kinds, shard_rows, orbitals), float32),
            pltpu.VMEM((2, perturbations, block_rows, shard_rows), float32),
            pltpu.SemaphoreType.DMA((8, pieces)),
            pltpu.SemaphoreType.DMA((4 * pieces,)),
            pltpu.SemaphoreType.DMA((7,)),
            pltpu.SemaphoreType.DMA((2,)),
            pltpu.SemaphoreType.DMA((2,)),
        ],
        compiler_params=pltpu.CompilerParams(
            collective_id=0, has_side_effects=True, vmem_limit_bytes=66_000_000
        ),
    )(response_coeffs, occupied_coeffs)[0]


def solution(mesh):
    fits = mesh.shape["row"] == 4 and mesh.shape["col"] == 8
    return jax.shard_map(
        panels if fits else shards,
        mesh=mesh,
        in_specs=(P(None, ("row", "col"), None), P(("row", "col"), None)),
        out_specs=P(None, "row", "col"),
        check_vma=False,
    )
```

```python
import functools

import jax
import jax.numpy as jnp
from jax import lax
from jax.experimental import pallas as pl
from jax.experimental.pallas import tpu as pltpu
from jax.sharding import PartitionSpec as P

SLICE_PAIRS = ((0, 0), (0, 1), (1, 0))


def partner(value, axis, stride):
    mask = 2**stride
    pairs = [(source, source ^ mask) for source in range(lax.axis_size(axis))]
    return lax.ppermute(value, axis, pairs)


def split_slices(values):
    leading = lax.optimization_barrier(values.astype(jnp.bfloat16))
    remainder = values - leading.astype(jnp.float32)
    trailing = lax.optimization_barrier(remainder.astype(jnp.bfloat16))
    return [leading, trailing]


def contribute(row_slices, column_slices, perturbations):
    accumulated = jnp.zeros(
        (perturbations, row_slices[0].shape[1], column_slices[0].shape[1]), jnp.float32
    )
    for left_index, right_index in SLICE_PAIRS:
        forward_term = jnp.einsum(
            "kro,co->krc",
            row_slices[left_index][:perturbations],
            column_slices[right_index][perturbations],
            preferred_element_type=jnp.float32,
        )
        mirror_term = jnp.einsum(
            "ro,kco->krc",
            row_slices[right_index][perturbations],
            column_slices[left_index][:perturbations],
            preferred_element_type=jnp.float32,
        )
        accumulated = accumulated + forward_term + mirror_term
    return accumulated


def relay_columns(stacked, perturbations):
    rows_total = lax.axis_size("row")
    columns_total = lax.axis_size("col")
    col_index = lax.axis_index("col")
    shard_rows = stacked.shape[1]
    orbitals = stacked.shape[2]
    half_rows = shard_rows // 2
    swap_bit = rows_total.bit_length() - 1
    own_first = stacked[:, :half_rows]
    partner_second = partner(stacked[:, half_rows:], "col", swap_bit)
    even_first = col_index // rows_total == 0
    leading = jnp.where(even_first, own_first, partner_second)
    trailing = jnp.where(even_first, partner_second, own_first)
    paired = jnp.concatenate([leading, trailing], axis=1)
    gathered = lax.all_gather(paired, "row", axis=1, tiled=True)
    regrouped = lax.all_to_all(gathered, "col", split_axis=1, concat_axis=1, tiled=True)
    shaped = regrouped.reshape(perturbations + 1, 2, rows_total, half_rows, orbitals)
    flipped = shaped[:, ::-1]
    ordered = jnp.where(col_index % 2 == 0, shaped, flipped)
    return jnp.swapaxes(ordered, 1, 2).reshape(
        perturbations + 1, columns_total * half_rows, orbitals
    )


def shards(response_coeffs, occupied_coeffs):
    perturbations = response_coeffs.shape[0]
    stacked = jnp.concatenate([response_coeffs, occupied_coeffs[None]], axis=0)
    column_panel = relay_columns(stacked, perturbations)
    column_slices = split_slices(column_panel)
    return contribute(
        split_slices(lax.all_gather(stacked, "col", axis=1, tiled=True)),
        column_slices,
        perturbations,
    )


HALVES = 2


def flip(value):
    return value + 1 - 2 * (value % 2)


def across(value):
    return value + 2 - 4 * (value // 2)


def panel_kernel(
    resp, occ, out, rowbuf, colbuf, latebuf,
    row_lead, row_trail, col_lead, col_trail, stage, tile,
    rx_row, rx_col, rx_late, tx, stage_sem, tile_sem,
):
    perturbations, shard_rows, orbitals = resp.shape
    kinds = perturbations + 1
    piece = shard_rows // HALVES
    pieces = kinds * HALVES
    early = pieces // 2
    positions = 4 * pieces
    block_rows = tile.shape[2]
    row_blocks = 8 * shard_rows // block_rows
    panel_rows = 8 * shard_rows

    z = lax.axis_index("row")
    planes = lax.axis_size("row")
    column = lax.axis_index("col")
    w, core = column // 2, column % 2
    xq, yq, dq = flip(w), across(w), flip(across(w))
    other = 1 - core
    x_dev, y_dev, p_dev = (z, 2 * xq + core), (z, 2 * yq + core), (z, 2 * w + other)
    up_dev, down_dev = (z + 1, column), (z - 1, column)
    has_up, has_down = z < planes - 1, z > 0
    diagonal = z == w
    match = w // 2 == core
    distance = jnp.where(z > w, z - w, w - z)

    barrier = pltpu.get_barrier_semaphore()

    def greet(device):
        pl.semaphore_signal(barrier, inc=1, device_id=device, device_id_type=pl.DeviceIdType.MESH)

    for offset in range(1, 8):
        greet((z, (column + offset) % 8))
    for offset in (1, planes - 1):
        greet(((z + offset) % planes, column))
    pl.semaphore_wait(barrier, 9)

    low, high = w == 0, w == planes - 1
    relay = low | high
    depth = jnp.where(low, planes - 1 - z, z)
    onward = jnp.where(low, has_down, has_up)
    onward_dev = (jnp.where(low, jnp.maximum(z - 1, 0), jnp.minimum(z + 1, planes - 1)), column)
    late_in = ((z < w) & (core == 0)) | ((z > w) & (core == 1))

    def row_piece(quarter, lane, j):
        return rowbuf.at[2 * quarter + lane, j // HALVES, pl.ds(pl.multiple_of((j % HALVES) * piece, piece), piece)]

    def col_piece(p):
        i, j = p // pieces, p % pieces
        return colbuf.at[i, j // HALVES, pl.ds(pl.multiple_of((j % HALVES) * piece, piece), piece)]

    def late_piece(m, j):
        return latebuf.at[m, j // HALVES, pl.ds(pl.multiple_of((j % HALVES) * piece, piece), piece)]

    def send(source, target, send_sem, recv_sem, device):
        pltpu.make_async_remote_copy(
            src_ref=source, dst_ref=target, send_sem=send_sem, recv_sem=recv_sem,
            device_id=device, device_id_type=pl.DeviceIdType.MESH,
        ).start()

    def send_row(quarter, lane, j, slot, device):
        ref = row_piece(quarter, lane, j)
        send(ref, ref, tx.at[slot], rx_row.at[2 * quarter + lane, j], device)

    def wait_row(quarter, lane, j):
        ref = row_piece(quarter, lane, j)
        pltpu.make_async_copy(ref, ref, rx_row.at[2 * quarter + lane, j]).wait()

    load_resp = pltpu.make_async_copy(resp, stage.at[pl.ds(0, perturbations)], stage_sem.at[0])
    load_occ = pltpu.make_async_copy(occ, stage.at[perturbations], stage_sem.at[1])
    load_resp.start()
    load_occ.start()
    for j in range(pieces):
        k, rows = j // HALVES, pl.ds((j % HALVES) * piece, piece)
        source = resp.at[k, rows] if k < perturbations else occ.at[rows]
        for slot, device in ((0, x_dev), (1, y_dev), (4, p_dev)):
            send(source, row_piece(w, core, j), tx.at[slot], rx_row.at[2 * w + core, j], device)
    load_resp.wait()
    load_occ.wait()
    keep = pltpu.make_async_copy(stage, rowbuf.at[2 * w + core], stage_sem.at[0])
    keep.start()
    keep.wait()

    full_first = jnp.where(match, w, yq)
    lone = jnp.where(core == 0, 1, 2)
    first = jnp.where(late_in, lone, full_first)

    def sequence(lead, i):
        quarter = jnp.where(i < 2, lead, flip(lead))
        lane = jnp.where(i % 2 == 0, core, other)
        return quarter, lane

    def order(i):
        return sequence(first, i)

    def position(quarter, lane, j):
        return (2 * (quarter % 2) + lane) * pieces + j

    def emit(source, p, upward):
        if upward:
            send(source, col_piece(p), tx.at[5], rx_col.at[p], up_dev)
        else:
            send(source, col_piece(p), tx.at[6], rx_col.at[p], down_dev)

    def emit_own(lead, n, upward):
        quarter, lane = sequence(lead, n // pieces)
        emit(row_piece(quarter, lane, n % pieces), position(quarter, lane, n % pieces), upward)

    def originate(t, upward, single):
        def at(condition, lead, base, count, pace):
            @pl.when(condition & (t >= base) & (t < base + count // pace))
            def _():
                for extra in range(pace):
                    emit_own(lead, pace * (t - base) + extra, upward)

        here = diagonal & (has_up if upward else has_down)
        alone = core == single
        at(here & (core != single) & match, full_first, 0, positions, 2)
        at(here & (core != single) & (w // 2 != core), full_first, 0, positions, 1)
        at(here & alone & (lone == w), lone, 0, positions // 2, 2)
        at(here & alone & (lone == yq), lone, 0, positions // 2, 1)
        at(here & alone & (lone == dq), lone, gathered, positions // 2, 2)

    def split_into(value, lead, trail, start):
        leading = value.astype(jnp.bfloat16)
        lead[pl.ds(start, shard_rows), :] = leading
        trail[pl.ds(start, shard_rows), :] = (value - leading.astype(jnp.float32)).astype(jnp.bfloat16)

    def load_stage(source):
        copy = pltpu.make_async_copy(source, stage, stage_sem.at[0])
        copy.start()
        copy.wait()

    def tile_copy(slot, block, start):
        return pltpu.make_async_copy(
            tile.at[slot],
            out.at[:, pl.ds(pl.multiple_of(block * block_rows, block_rows), block_rows),
                   pl.ds(pl.multiple_of(start, shard_rows), shard_rows)],
            tile_sem.at[slot],
        )

    gathered = pieces + early
    convert_at = gathered + 1
    matmul_at = convert_at + 8
    rounds = positions + planes - 1
    hidden = 3 * row_blocks
    tasks = 4 * row_blocks

    def step(t, carry):
        @pl.when(t < pieces)
        def _():
            wait_row(xq, core, t)
            send_row(xq, core, t, 4, p_dev)
            wait_row(yq, core, t)
            send_row(yq, core, t, 4, p_dev)
            wait_row(w, other, t)

            @pl.when(t < early)
            def _():
                send_row(yq, core, t, 2, x_dev)

            @pl.when(t >= early)
            def _():
                send_row(xq, core, t, 3, y_dev)

        @pl.when((t >= 1) & (t < pieces + 1))
        def _():
            wait_row(xq, other, t - 1)
            wait_row(yq, other, t - 1)

        @pl.when((t >= pieces) & (t < gathered))
        def _():
            for shift in (0, early):
                wait_row(dq, core, t - pieces + shift)
                send_row(dq, core, t - pieces + shift, 4, p_dev)

        @pl.when((t >= pieces + 1) & (t < gathered + 1))
        def _():
            for shift in (0, early):
                wait_row(dq, other, t - pieces - 1 + shift)

        originate(t, True, 1)
        originate(t, False, 0)

        arriving = jnp.where(late_in, positions // 2, positions)

        @pl.when((z != w) & (t >= distance) & (t < arriving + distance))
        def _():
            n = t - distance
            quarter, lane = order(n // pieces)
            p = position(quarter, lane, n % pieces)
            ref = col_piece(p)
            pltpu.make_async_copy(ref, ref, rx_col.at[p]).wait()

            @pl.when(has_up & (z > w))
            def _():
                emit(ref, p, True)

            @pl.when(has_down & (z < w))
            def _():
                emit(ref, p, False)

        own_at = jnp.where(depth > 0, (pieces + 1) * depth - 1, 0)

        @pl.when(relay & onward & (t >= own_at) & (t < own_at + pieces))
        def _():
            j = t - own_at
            send(row_piece(w, core, j), late_piece(depth, j), tx.at[7 + depth], rx_late.at[depth, j], onward_dev)

        @pl.when(relay & (t + 1 >= depth) & (t + 1 < depth + pieces * depth))
        def _():
            n = t + 1 - depth
            m, j = n // pieces, n % pieces
            ref = late_piece(m, j)
            pltpu.make_async_copy(ref, ref, rx_late.at[m, j]).wait()

            @pl.when(onward)
            def _():
                send(ref, ref, tx.at[7 + m], rx_late.at[m, j], onward_dev)

            panel = jnp.where(low, planes - 1 - m, m)
            side = jnp.where(low, 0, 1)
            p = position(w, core, j)
            send(ref, col_piece(p), tx.at[11 + m], rx_col.at[p], (z, 2 * panel + side))

        @pl.when((t >= convert_at) & (t < matmul_at))
        def _():
            shard = t - convert_at
            load_stage(rowbuf.at[shard])

            def convert(k, carry):
                start = pl.multiple_of(k * panel_rows + shard * shard_rows, shard_rows)
                split_into(stage[k], row_lead, row_trail, start)
                return carry

            lax.fori_loop(0, kinds, convert, 0)

        @pl.when(((t >= matmul_at) & (t < matmul_at + hidden)) | (t >= rounds))
        def _():
            task = jnp.where(t >= rounds, t - rounds + hidden, t - matmul_at)
            part, block = task // row_blocks, task % row_blocks
            quarter, lane = order(part)

            @pl.when(block == 0)
            def _():
                @pl.when(diagonal)
                def _():
                    load_stage(rowbuf.at[2 * quarter + lane])

                @pl.when(z != w)
                def _():
                    shard = 2 * (quarter % 2) + lane

                    @pl.when(late_in & (part >= 2))
                    def _():
                        def arrive(j, carry):
                            p = position(quarter, lane, j)
                            ref = col_piece(p)
                            pltpu.make_async_copy(ref, ref, rx_col.at[p]).wait()
                            return carry

                        lax.fori_loop(0, pieces, arrive, 0)

                    load_stage(colbuf.at[shard])

                def convert(k, carry):
                    split_into(stage[k], col_lead, col_trail, pl.multiple_of(k * shard_rows, shard_rows))
                    return carry

                lax.fori_loop(0, kinds, convert, 0)

            slot = task % 2
            place = (2 * (quarter % 2) + lane) * shard_rows

            @pl.when(task >= 2)
            def _():
                tile_copy(slot, block, place).wait()

            def rows_of(ref, k):
                return ref[pl.ds(pl.multiple_of(k * panel_rows + block * block_rows, block_rows), block_rows), :]

            def columns_of(ref, k):
                return ref[pl.ds(pl.multiple_of(k * shard_rows, shard_rows), shard_rows), :]

            def product(left, right):
                return lax.dot_general(left, right, (((1,), (1,)), ((), ())), preferred_element_type=jnp.float32)

            def perturbation(k, carry):
                total = product(rows_of(row_lead, k), columns_of(col_lead, perturbations))
                total += product(rows_of(row_lead, k), columns_of(col_trail, perturbations))
                total += product(rows_of(row_trail, k), columns_of(col_lead, perturbations))
                total += product(rows_of(row_lead, perturbations), columns_of(col_lead, k))
                total += product(rows_of(row_trail, perturbations), columns_of(col_lead, k))
                total += product(rows_of(row_lead, perturbations), columns_of(col_trail, k))
                tile[slot, k] = total
                return carry

            lax.fori_loop(0, perturbations, perturbation, 0)
            tile_copy(slot, block, place).start()

        return carry

    lax.fori_loop(0, rounds + row_blocks, step, 0)

    for slot in range(2):
        tile_copy(slot, 0, 0).wait()

    def drain(slot, ref):
        pltpu.make_async_copy(ref, ref, tx.at[slot]).wait()

    drain(0, rowbuf.at[0])
    drain(1, rowbuf.at[0])
    drain(2, rowbuf.at[0, pl.ds(0, kinds // 2)])
    drain(3, rowbuf.at[0, pl.ds(0, kinds // 2)])
    drain(4, rowbuf.at[pl.ds(0, 4)])

    for slot, single, sends in ((5, 1, has_up & (z >= w)), (6, 0, has_down & (z <= w))):
        @pl.when(sends & (core != single))
        def _():
            drain(slot, rowbuf.at[pl.ds(0, 4)])

        @pl.when(sends & (core == single))
        def _():
            drain(slot, rowbuf.at[pl.ds(0, 2)])

    for m in range(4):
        @pl.when(relay & onward & (m <= depth))
        def _():
            drain(7 + m, rowbuf.at[0])

    for m in range(3):
        @pl.when(relay & (m < depth))
        def _():
            drain(11 + m, rowbuf.at[0])


def panels(response_coeffs, occupied_coeffs):
    perturbations, shard_rows, orbitals = response_coeffs.shape
    kinds = perturbations + 1
    pieces = kinds * HALVES
    block_rows = 2 * shard_rows
    any_space = pl.BlockSpec(memory_space=pl.ANY)
    float32, bfloat16 = jnp.float32, jnp.bfloat16
    return pl.pallas_call(
        panel_kernel,
        out_shape=(
            jax.ShapeDtypeStruct((perturbations, 8 * shard_rows, 4 * shard_rows), float32),
            jax.ShapeDtypeStruct((8, kinds, shard_rows, orbitals), float32),
            jax.ShapeDtypeStruct((4, kinds, shard_rows, orbitals), float32),
            jax.ShapeDtypeStruct((3, kinds, shard_rows, orbitals), float32),
        ),
        in_specs=[any_space] * 2,
        out_specs=(any_space,) * 4,
        scratch_shapes=[
            pltpu.VMEM((kinds * 8 * shard_rows, orbitals), bfloat16),
            pltpu.VMEM((kinds * 8 * shard_rows, orbitals), bfloat16),
            pltpu.VMEM((kinds * shard_rows, orbitals), bfloat16),
            pltpu.VMEM((kinds * shard_rows, orbitals), bfloat16),
            pltpu.VMEM((kinds, shard_rows, orbitals), float32),
            pltpu.VMEM((2, perturbations, block_rows, shard_rows), float32),
            pltpu.SemaphoreType.DMA((8, pieces)),
            pltpu.SemaphoreType.DMA((4 * pieces,)),
            pltpu.SemaphoreType.DMA((3, pieces)),
            pltpu.SemaphoreType.DMA((14,)),
            pltpu.SemaphoreType.DMA((2,)),
            pltpu.SemaphoreType.DMA((2,)),
        ],
        compiler_params=pltpu.CompilerParams(
            collective_id=0, has_side_effects=True, vmem_limit_bytes=66_000_000
        ),
    )(response_coeffs, occupied_coeffs)[0]


def solution(mesh):
    fits = mesh.shape["row"] == 4 and mesh.shape["col"] == 8
    return jax.shard_map(
        panels if fits else shards,
        mesh=mesh,
        in_specs=(P(None, ("row", "col"), None), P(("row", "col"), None)),
        out_specs=P(None, "row", "col"),
        check_vma=False,
    )
```

```python
import functools

import jax
import jax.numpy as jnp
from jax import lax
from jax.experimental import pallas as pl
from jax.experimental.pallas import tpu as pltpu
from jax.sharding import PartitionSpec as P

SLICE_PAIRS = ((0, 0), (0, 1), (1, 0))


def partner(value, axis, stride):
    mask = 2**stride
    pairs = [(source, source ^ mask) for source in range(lax.axis_size(axis))]
    return lax.ppermute(value, axis, pairs)


def split_slices(values):
    leading = lax.optimization_barrier(values.astype(jnp.bfloat16))
    remainder = values - leading.astype(jnp.float32)
    trailing = lax.optimization_barrier(remainder.astype(jnp.bfloat16))
    return [leading, trailing]


def contribute(row_slices, column_slices, perturbations):
    accumulated = jnp.zeros(
        (perturbations, row_slices[0].shape[1], column_slices[0].shape[1]), jnp.float32
    )
    for left_index, right_index in SLICE_PAIRS:
        forward_term = jnp.einsum(
            "kro,co->krc",
            row_slices[left_index][:perturbations],
            column_slices[right_index][perturbations],
            preferred_element_type=jnp.float32,
        )
        mirror_term = jnp.einsum(
            "ro,kco->krc",
            row_slices[right_index][perturbations],
            column_slices[left_index][:perturbations],
            preferred_element_type=jnp.float32,
        )
        accumulated = accumulated + forward_term + mirror_term
    return accumulated


def relay_columns(stacked, perturbations):
    rows_total = lax.axis_size("row")
    columns_total = lax.axis_size("col")
    col_index = lax.axis_index("col")
    shard_rows = stacked.shape[1]
    orbitals = stacked.shape[2]
    half_rows = shard_rows // 2
    swap_bit = rows_total.bit_length() - 1
    own_first = stacked[:, :half_rows]
    partner_second = partner(stacked[:, half_rows:], "col", swap_bit)
    even_first = col_index // rows_total == 0
    leading = jnp.where(even_first, own_first, partner_second)
    trailing = jnp.where(even_first, partner_second, own_first)
    paired = jnp.concatenate([leading, trailing], axis=1)
    gathered = lax.all_gather(paired, "row", axis=1, tiled=True)
    regrouped = lax.all_to_all(gathered, "col", split_axis=1, concat_axis=1, tiled=True)
    shaped = regrouped.reshape(perturbations + 1, 2, rows_total, half_rows, orbitals)
    flipped = shaped[:, ::-1]
    ordered = jnp.where(col_index % 2 == 0, shaped, flipped)
    return jnp.swapaxes(ordered, 1, 2).reshape(
        perturbations + 1, columns_total * half_rows, orbitals
    )


def shards(response_coeffs, occupied_coeffs):
    perturbations = response_coeffs.shape[0]
    stacked = jnp.concatenate([response_coeffs, occupied_coeffs[None]], axis=0)
    column_panel = relay_columns(stacked, perturbations)
    column_slices = split_slices(column_panel)
    return contribute(
        split_slices(lax.all_gather(stacked, "col", axis=1, tiled=True)),
        column_slices,
        perturbations,
    )


HALVES = 2
LAG = 2


def flip(value):
    return value + 1 - 2 * (value % 2)


def across(value):
    return value + 2 - 4 * (value // 2)


def panel_kernel(
    resp, occ, out, rowbuf, colbuf, latebuf,
    row_lead, row_trail, col_lead, col_trail, stage, tile,
    rx_row, rx_col, rx_late, tx, stage_sem, tile_sem,
):
    perturbations, shard_rows, orbitals = resp.shape
    kinds = perturbations + 1
    piece = shard_rows // HALVES
    pieces = kinds * HALVES
    early = pieces // 2
    positions = 4 * pieces
    block_rows = tile.shape[2]
    row_blocks = 8 * shard_rows // block_rows
    panel_rows = 8 * shard_rows

    z = lax.axis_index("row")
    planes = lax.axis_size("row")
    column = lax.axis_index("col")
    w, core = column // 2, column % 2
    xq, yq, dq = flip(w), across(w), flip(across(w))
    other = 1 - core
    x_dev, y_dev, p_dev = (z, 2 * xq + core), (z, 2 * yq + core), (z, 2 * w + other)
    up_dev, down_dev = (z + 1, column), (z - 1, column)
    has_up, has_down = z < planes - 1, z > 0
    diagonal = z == w
    match = w // 2 == core
    distance = LAG * jnp.where(z > w, z - w, w - z)

    barrier = pltpu.get_barrier_semaphore()

    def greet(device):
        pl.semaphore_signal(barrier, inc=1, device_id=device, device_id_type=pl.DeviceIdType.MESH)

    for offset in range(1, 8):
        greet((z, (column + offset) % 8))
    for offset in (1, planes - 1):
        greet(((z + offset) % planes, column))
    pl.semaphore_wait(barrier, 9)

    low, high = w == 0, w == planes - 1
    relay = low | high
    depth = jnp.where(low, planes - 1 - z, z)
    onward = jnp.where(low, has_down, has_up)
    onward_dev = (jnp.where(low, jnp.maximum(z - 1, 0), jnp.minimum(z + 1, planes - 1)), column)
    late_in = ((z < w) & (core == 0)) | ((z > w) & (core == 1))

    def row_piece(quarter, lane, j):
        return rowbuf.at[2 * quarter + lane, j // HALVES, pl.ds(pl.multiple_of((j % HALVES) * piece, piece), piece)]

    def col_piece(p):
        i, j = p // pieces, p % pieces
        return colbuf.at[i, j // HALVES, pl.ds(pl.multiple_of((j % HALVES) * piece, piece), piece)]

    def late_piece(m, j):
        return latebuf.at[m, j // HALVES, pl.ds(pl.multiple_of((j % HALVES) * piece, piece), piece)]

    def send(source, target, send_sem, recv_sem, device):
        pltpu.make_async_remote_copy(
            src_ref=source, dst_ref=target, send_sem=send_sem, recv_sem=recv_sem,
            device_id=device, device_id_type=pl.DeviceIdType.MESH,
        ).start()

    def send_row(quarter, lane, j, slot, device):
        ref = row_piece(quarter, lane, j)
        send(ref, ref, tx.at[slot], rx_row.at[2 * quarter + lane, j], device)

    def wait_row(quarter, lane, j):
        ref = row_piece(quarter, lane, j)
        pltpu.make_async_copy(ref, ref, rx_row.at[2 * quarter + lane, j]).wait()

    load_resp = pltpu.make_async_copy(resp, stage.at[pl.ds(0, perturbations)], stage_sem.at[0])
    load_occ = pltpu.make_async_copy(occ, stage.at[perturbations], stage_sem.at[1])
    load_resp.start()
    load_occ.start()
    for j in range(pieces):
        k, rows = j // HALVES, pl.ds((j % HALVES) * piece, piece)
        source = resp.at[k, rows] if k < perturbations else occ.at[rows]
        for slot, device in ((0, x_dev), (1, y_dev), (4, p_dev)):
            send(source, row_piece(w, core, j), tx.at[slot], rx_row.at[2 * w + core, j], device)
    load_resp.wait()
    load_occ.wait()
    keep = pltpu.make_async_copy(stage, rowbuf.at[2 * w + core], stage_sem.at[0])
    keep.start()
    keep.wait()

    full_first = jnp.where(match, w, yq)
    lone = jnp.where(core == 0, 1, 2)
    first = jnp.where(late_in, lone, full_first)

    def sequence(lead, i):
        quarter = jnp.where(i < 2, lead, flip(lead))
        lane = jnp.where(i % 2 == 0, core, other)
        return quarter, lane

    def order(i):
        return sequence(first, i)

    def position(quarter, lane, j):
        return (2 * (quarter % 2) + lane) * pieces + j

    def emit(source, p, upward):
        if upward:
            send(source, col_piece(p), tx.at[5], rx_col.at[p], up_dev)
        else:
            send(source, col_piece(p), tx.at[6], rx_col.at[p], down_dev)

    def emit_own(lead, n, upward):
        quarter, lane = sequence(lead, n // pieces)
        emit(row_piece(quarter, lane, n % pieces), position(quarter, lane, n % pieces), upward)

    def originate(t, upward, single):
        def at(condition, lead, base, count, pace):
            @pl.when(condition & (t >= base) & (t < base + count // pace))
            def _():
                for extra in range(pace):
                    emit_own(lead, pace * (t - base) + extra, upward)

        here = diagonal & (has_up if upward else has_down)
        alone = core == single
        at(here & (core != single) & match, full_first, 0, positions, 2)
        at(here & (core != single) & (w // 2 != core), full_first, 0, positions, 1)
        at(here & alone & (lone == w), lone, 0, positions // 2, 2)
        at(here & alone & (lone == yq), lone, 0, positions // 2, 1)
        at(here & alone & (lone == dq), lone, gathered, positions // 2, 2)

    def split_into(value, lead, trail, start):
        leading = value.astype(jnp.bfloat16)
        lead[pl.ds(start, shard_rows), :] = leading
        trail[pl.ds(start, shard_rows), :] = (value - leading.astype(jnp.float32)).astype(jnp.bfloat16)

    def load_stage(source):
        copy = pltpu.make_async_copy(source, stage, stage_sem.at[0])
        copy.start()
        copy.wait()

    def tile_copy(slot, block, start):
        return pltpu.make_async_copy(
            tile.at[slot],
            out.at[:, pl.ds(pl.multiple_of(block * block_rows, block_rows), block_rows),
                   pl.ds(pl.multiple_of(start, shard_rows), shard_rows)],
            tile_sem.at[slot],
        )

    gathered = pieces + early
    convert_at = gathered + 1
    matmul_at = convert_at + 8
    rounds = positions + LAG * (planes - 1)
    hidden = 3 * row_blocks
    tasks = 4 * row_blocks

    def step(t, carry):
        @pl.when(t < pieces)
        def _():
            wait_row(xq, core, t)
            send_row(xq, core, t, 4, p_dev)
            wait_row(yq, core, t)
            send_row(yq, core, t, 4, p_dev)
            wait_row(w, other, t)

            @pl.when(t < early)
            def _():
                send_row(yq, core, t, 2, x_dev)

            @pl.when(t >= early)
            def _():
                send_row(xq, core, t, 3, y_dev)

        @pl.when((t >= 1) & (t < pieces + 1))
        def _():
            wait_row(xq, other, t - 1)
            wait_row(yq, other, t - 1)

        @pl.when((t >= pieces) & (t < gathered))
        def _():
            for shift in (0, early):
                wait_row(dq, core, t - pieces + shift)
                send_row(dq, core, t - pieces + shift, 4, p_dev)

        @pl.when((t >= pieces + 1) & (t < gathered + 1))
        def _():
            for shift in (0, early):
                wait_row(dq, other, t - pieces - 1 + shift)

        originate(t, True, 1)
        originate(t, False, 0)

        arriving = jnp.where(late_in, positions // 2, positions)

        @pl.when((z != w) & (t >= distance) & (t < arriving + distance))
        def _():
            n = t - distance
            quarter, lane = order(n // pieces)
            p = position(quarter, lane, n % pieces)
            ref = col_piece(p)
            pltpu.make_async_copy(ref, ref, rx_col.at[p]).wait()

            @pl.when(has_up & (z > w))
            def _():
                emit(ref, p, True)

            @pl.when(has_down & (z < w))
            def _():
                emit(ref, p, False)

        own_at = (pieces + LAG) * depth

        @pl.when(relay & onward & (t >= own_at) & (t < own_at + pieces))
        def _():
            j = t - own_at
            send(row_piece(w, core, j), late_piece(depth, j), tx.at[7 + depth], rx_late.at[depth, j], onward_dev)

        @pl.when(relay & (t >= LAG * depth) & (t < (LAG + pieces) * depth))
        def _():
            n = t - LAG * depth
            m, j = n // pieces, n % pieces
            ref = late_piece(m, j)
            pltpu.make_async_copy(ref, ref, rx_late.at[m, j]).wait()

            @pl.when(onward)
            def _():
                send(ref, ref, tx.at[7 + m], rx_late.at[m, j], onward_dev)

            panel = jnp.where(low, planes - 1 - m, m)
            side = jnp.where(low, 0, 1)
            p = position(w, core, j)
            send(ref, col_piece(p), tx.at[11 + m], rx_col.at[p], (z, 2 * panel + side))

        @pl.when((t >= convert_at) & (t < matmul_at))
        def _():
            shard = t - convert_at
            load_stage(rowbuf.at[shard])

            def convert(k, carry):
                start = pl.multiple_of(k * panel_rows + shard * shard_rows, shard_rows)
                split_into(stage[k], row_lead, row_trail, start)
                return carry

            lax.fori_loop(0, kinds, convert, 0)

        @pl.when(((t >= matmul_at) & (t < matmul_at + hidden)) | (t >= rounds))
        def _():
            task = jnp.where(t >= rounds, t - rounds + hidden, t - matmul_at)
            part, block = task // row_blocks, task % row_blocks
            quarter, lane = order(part)

            @pl.when(block == 0)
            def _():
                @pl.when(diagonal)
                def _():
                    load_stage(rowbuf.at[2 * quarter + lane])

                @pl.when(z != w)
                def _():
                    shard = 2 * (quarter % 2) + lane

                    @pl.when(late_in & (part >= 2))
                    def _():
                        def arrive(j, carry):
                            p = position(quarter, lane, j)
                            ref = col_piece(p)
                            pltpu.make_async_copy(ref, ref, rx_col.at[p]).wait()
                            return carry

                        lax.fori_loop(0, pieces, arrive, 0)

                    load_stage(colbuf.at[shard])

                def convert(k, carry):
                    split_into(stage[k], col_lead, col_trail, pl.multiple_of(k * shard_rows, shard_rows))
                    return carry

                lax.fori_loop(0, kinds, convert, 0)

            slot = task % 2
            place = (2 * (quarter % 2) + lane) * shard_rows

            @pl.when(task >= 2)
            def _():
                tile_copy(slot, block, place).wait()

            def rows_of(ref, k):
                return ref[pl.ds(pl.multiple_of(k * panel_rows + block * block_rows, block_rows), block_rows), :]

            def columns_of(ref, k):
                return ref[pl.ds(pl.multiple_of(k * shard_rows, shard_rows), shard_rows), :]

            def product(left, right):
                return lax.dot_general(left, right, (((1,), (1,)), ((), ())), preferred_element_type=jnp.float32)

            def perturbation(k, carry):
                total = product(rows_of(row_lead, k), columns_of(col_lead, perturbations))
                total += product(rows_of(row_lead, k), columns_of(col_trail, perturbations))
                total += product(rows_of(row_trail, k), columns_of(col_lead, perturbations))
                total += product(rows_of(row_lead, perturbations), columns_of(col_lead, k))
                total += product(rows_of(row_trail, perturbations), columns_of(col_lead, k))
                total += product(rows_of(row_lead, perturbations), columns_of(col_trail, k))
                tile[slot, k] = total
                return carry

            lax.fori_loop(0, perturbations, perturbation, 0)
            tile_copy(slot, block, place).start()

        return carry

    lax.fori_loop(0, rounds + row_blocks, step, 0)

    for slot in range(2):
        tile_copy(slot, 0, 0).wait()

    def drain(slot, ref):
        pltpu.make_async_copy(ref, ref, tx.at[slot]).wait()

    drain(0, rowbuf.at[0])
    drain(1, rowbuf.at[0])
    drain(2, rowbuf.at[0, pl.ds(0, kinds // 2)])
    drain(3, rowbuf.at[0, pl.ds(0, kinds // 2)])
    drain(4, rowbuf.at[pl.ds(0, 4)])

    for slot, single, sends in ((5, 1, has_up & (z >= w)), (6, 0, has_down & (z <= w))):
        @pl.when(sends & (core != single))
        def _():
            drain(slot, rowbuf.at[pl.ds(0, 4)])

        @pl.when(sends & (core == single))
        def _():
            drain(slot, rowbuf.at[pl.ds(0, 2)])

    for m in range(4):
        @pl.when(relay & onward & (m <= depth))
        def _():
            drain(7 + m, rowbuf.at[0])

    for m in range(3):
        @pl.when(relay & (m < depth))
        def _():
            drain(11 + m, rowbuf.at[0])


def panels(response_coeffs, occupied_coeffs):
    perturbations, shard_rows, orbitals = response_coeffs.shape
    kinds = perturbations + 1
    pieces = kinds * HALVES
    block_rows = 2 * shard_rows
    any_space = pl.BlockSpec(memory_space=pl.ANY)
    float32, bfloat16 = jnp.float32, jnp.bfloat16
    return pl.pallas_call(
        panel_kernel,
        out_shape=(
            jax.ShapeDtypeStruct((perturbations, 8 * shard_rows, 4 * shard_rows), float32),
            jax.ShapeDtypeStruct((8, kinds, shard_rows, orbitals), float32),
            jax.ShapeDtypeStruct((4, kinds, shard_rows, orbitals), float32),
            jax.ShapeDtypeStruct((3, kinds, shard_rows, orbitals), float32),
        ),
        in_specs=[any_space] * 2,
        out_specs=(any_space,) * 4,
        scratch_shapes=[
            pltpu.VMEM((kinds * 8 * shard_rows, orbitals), bfloat16),
            pltpu.VMEM((kinds * 8 * shard_rows, orbitals), bfloat16),
            pltpu.VMEM((kinds * shard_rows, orbitals), bfloat16),
            pltpu.VMEM((kinds * shard_rows, orbitals), bfloat16),
            pltpu.VMEM((kinds, shard_rows, orbitals), float32),
            pltpu.VMEM((2, perturbations, block_rows, shard_rows), float32),
            pltpu.SemaphoreType.DMA((8, pieces)),
            pltpu.SemaphoreType.DMA((4 * pieces,)),
            pltpu.SemaphoreType.DMA((3, pieces)),
            pltpu.SemaphoreType.DMA((14,)),
            pltpu.SemaphoreType.DMA((2,)),
            pltpu.SemaphoreType.DMA((2,)),
        ],
        compiler_params=pltpu.CompilerParams(
            collective_id=0, has_side_effects=True, vmem_limit_bytes=66_000_000
        ),
    )(response_coeffs, occupied_coeffs)[0]


def solution(mesh):
    fits = mesh.shape["row"] == 4 and mesh.shape["col"] == 8
    return jax.shard_map(
        panels if fits else shards,
        mesh=mesh,
        in_specs=(P(None, ("row", "col"), None), P(("row", "col"), None)),
        out_specs=P(None, "row", "col"),
        check_vma=False,
    )
```
